32 devices in a mesh: dp: 8 (over y, x, core), tensor: 4 (over z).
Axes of the slice: x: 2, y: 2, z: 4, core: 2. Of those that a mesh axis runs over, the one named last changes fastest.
Arguments:
- hidden_in: bfloat16 [8, 128, 16384], P('dp'), may hold values from -6 to 6
- value_weight: bfloat16 [16384, 256], P(None, 'tensor'), may hold values from -0.046875 to 0.046875
- queries: bfloat16 [8, 128, 4096], P('dp', None, 'tensor'), may hold values from -4 to 4
- key_rows: bfloat16 [8, 128, 256], P('dp', None, 'tensor'), may hold values from -4 to 4
- attention_out: bfloat16 [8, 128, 4096], P('dp', None, 'tensor'), may hold values from -4 to 4
- output_grad: bfloat16 [8, 128, 4096], P('dp', None, 'tensor'), may hold values from -6 to 6
- log_normalizer: float32 [8, 128, 32], P('dp', None, 'tensor'), may hold values from 1 to 5
- document_ids: int32 [8, 128], P('dp'), may hold values from 0 to 3, never falling along the last dimension, each value on 1 to 64 neighbouring positions
Outputs:
- query_grad: bfloat16 [8, 128, 4096], P('dp', None, 'tensor')
- key_grad: bfloat16 [8, 128, 256], P('dp', None, 'tensor')
- input_grad: bfloat16 [8, 128, 16384], P('dp', 'tensor')
- value_weight_grad: float32 [16384, 256], P('dp', 'tensor')
The draws below stay inside these ranges and needn't reach their ends.
Inputs may be any that keep to these rules, and one draw needn't show every extreme that they name: `document_ids`: within one group the ids never fall; all 4 documents occur, each of 1 to 64 tokens.
All inputs are finite; a program needn't handle non-finite values.
Results may differ from the reference program's by a relative error of at most 0.014.
Values may be sent and summed in bfloat16 or wider, within the bound.
No kernel may reach another device: no remote copies, remote signals or barrier semaphores. Data moves between devices by JAX's collectives and lax.ppermute only.
A program may use at most 64 MiB of HBM per device.

```python
import math
from functools import partial
import jax
import jax.numpy as jnp
import numpy as np
from jax import lax

D = 16384
HD = 128
GROUP = 16
TOK_DEV = 128
DOCS = 4
QHEADS = 32
KVH = 2
GROUPS = 8


def raised(values, own_key, source, target, shards_of, factor):
    owner, partner = [(jnp.arange(values.shape[dim]) // (values.shape[dim] // shards_of)).reshape([-1 if axis == dim else 1 for axis in range(values.ndim)]) for dim in (source, target)]
    chosen = jax.random.permutation(own_key, shards_of)[partner]
    strong = (owner == chosen) | (owner == (partner + shards_of // 2) % shards_of)
    return jnp.where(strong, factor * values, values)


def block_scale(stream_key, shape, pieces, smallest, high):
    level = 1.0
    for dim, parts in pieces:
        draws = jax.random.uniform(jax.random.fold_in(jax.random.fold_in(stream_key, 6), dim), (parts,), jnp.float32, smallest / len(pieces), high / len(pieces))
        level = level * jnp.repeat(jnp.exp(draws), shape[dim] // parts).reshape((-1,) + (1,) * (len(shape) - 1 - dim))
    return level


def profile(count, total, reach, lean):
    loads = [(1 << 20) // math.isqrt(grade ** lean) + 1 for grade in range(2, count + 1)]
    spare, counts = total - reach - (count - 1), [1] * (count - 1)
    while spare > 0:
        candidates = [i for i in range(count - 1) if counts[i] < reach]
        whole, budget = sum([loads[i] for i in candidates]), spare
        for i in candidates:
            addition = min(reach - counts[i], max(1, budget * loads[i] // whole), spare)
            counts[i] = counts[i] + addition
            spare = spare - addition
    return np.array([reach] + counts)


def uneven_parts(stream_key, amount, total, limit, skew):
    if amount == 2:
        one = jax.random.randint(stream_key, (), max(1, total - limit), min(limit, total - 1) + 1)
        return jnp.stack([one, total - one])
    sizes = jnp.asarray(profile(amount, total, limit, skew), jnp.int32)
    twos = (amount - 1) // 2
    source_of, sink = sizes[1:1 + 2 * twos:2], sizes[2:2 + 2 * twos:2]
    slack = jnp.minimum(source_of - 1, limit - sink)
    moved = jax.random.randint(jax.random.fold_in(stream_key, 1), (twos,), 0, 1 << 20) % (slack + 1)
    sizes = sizes.at[1:1 + 2 * twos:2].set(source_of - moved).at[2:2 + 2 * twos:2].set(sink + moved)
    return sizes[jax.random.permutation(jax.random.fold_in(stream_key, 2), amount)]


def gaussian(rng, extent, scale, reach, split=(), held_as=jnp.bfloat16):
    result = scale * jax.random.normal(rng, extent, jnp.float32)
    if split:
        result = result * block_scale(rng, extent, split, -0.22, 0.18)
    return jnp.clip(result, -reach, reach).astype(held_as)


def heavy_noise(key, dims, deviation, limit, split, heavy, kind=jnp.bfloat16):
    values = deviation * jax.random.normal(key, dims, jnp.float32)
    if split:
        values = values * block_scale(key, dims, split, -0.22, 0.18)
    return jnp.clip(raised(values, jax.random.fold_in(key, 3), *heavy), -limit, limit).astype(kind)


def setup_inputs(seed: int = 0) -> dict:
    keys = jax.random.split(jax.random.key(seed), 9)
    hidden_in = heavy_noise(keys[0], (GROUPS, TOK_DEV, D), 1.0, 6.0, ((0, 8),), (0, 2, 8, 2.0))
    value_weight = gaussian(keys[1], (D, KVH * HD), D ** -0.5, 0.046875, ((1, 4),))
    queries = gaussian(keys[2], (GROUPS, TOK_DEV, QHEADS * HD), 1.0, 4.0, ((0, 8), (2, 4)))
    key_rows = gaussian(keys[3], (GROUPS, TOK_DEV, KVH * HD), 1.0, 4.0, ((0, 8), (2, 4)))
    attention_out = gaussian(keys[4], (GROUPS, TOK_DEV, QHEADS * HD), 0.5, 4.0, ((0, 8), (2, 4)))
    output_grad = heavy_noise(keys[5], (GROUPS, TOK_DEV, QHEADS * HD), 1.0, 6.0, ((0, 8), (2, 4)), (2, 1, 4, 2.0))
    log_normalizer = jnp.clip(1.0 + 4.0 * jax.random.uniform(keys[6], (GROUPS, TOK_DEV, QHEADS), jnp.float32) ** block_scale(keys[6], (GROUPS, TOK_DEV, QHEADS), ((0, 8), (2, 4)), -0.2, 0.2), 1.0, 5.0)
    document_ids = jax.vmap(lambda own: jnp.searchsorted(jnp.cumsum(uneven_parts(own, DOCS, TOK_DEV, TOK_DEV // 2, 1)), jnp.arange(TOK_DEV), side="right"))(jax.random.split(keys[7], GROUPS)).reshape((GROUPS, TOK_DEV)).astype(jnp.int32)
    return {"hidden_in": hidden_in, "value_weight": value_weight, "queries": queries, "key_rows": key_rows, "attention_out": attention_out, "output_grad": output_grad, "log_normalizer": log_normalizer, "document_ids": document_ids}


def rounded(array):
    return lax.optimization_barrier(array.astype(jnp.bfloat16)).astype(jnp.float32)

def group_backward(value_weight, operands):
    hidden_in, queries, key_rows, attention_out, output_grad, log_normalizer, document_ids = operands
    tokens = hidden_in.shape[0]
    score_scale = 1.0 / math.sqrt(HD)
    values = jnp.dot(hidden_in, value_weight, preferred_element_type=jnp.float32).astype(jnp.bfloat16)
    query_heads = queries.astype(jnp.float32).reshape(tokens, KVH, GROUP, HD)
    key_heads = key_rows.astype(jnp.float32).reshape(tokens, KVH, HD)
    value_heads = values.astype(jnp.float32).reshape(tokens, KVH, HD)
    out_heads = attention_out.astype(jnp.float32).reshape(tokens, KVH, GROUP, HD)
    grad_heads = output_grad.astype(jnp.float32).reshape(tokens, KVH, GROUP, HD)
    normalizers = jnp.transpose(log_normalizer.reshape(tokens, KVH, GROUP), (1, 2, 0))[..., None]
    position = jnp.arange(tokens, dtype=jnp.int32)
    allowed = (position[None, :] <= position[:, None]) & (document_ids[:, None] == document_ids[None, :])
    scores = jnp.einsum('tcgd,scd->cgts', query_heads, key_heads) * score_scale
    probabilities = jnp.where(allowed, jnp.exp(scores - normalizers), 0.0)
    probs_low = rounded(probabilities)
    value_sum = jnp.einsum('cgts,tcgd->scd', probs_low, grad_heads)
    row_dots = jnp.einsum('tcgd,tcgd->cgt', grad_heads, out_heads)
    prob_grad = jnp.einsum('tcgd,scd->cgts', grad_heads, value_heads)
    score_grad = rounded(probabilities * (prob_grad - row_dots[..., None]) * score_scale)
    query_grad = jnp.einsum('cgts,scd->tcgd', score_grad, key_heads).astype(jnp.bfloat16)
    key_grad = jnp.einsum('cgts,tcgd->scd', score_grad, query_heads).astype(jnp.bfloat16)
    value_grad = value_sum.astype(jnp.bfloat16).reshape(tokens, KVH * HD)
    block_width = HD // 2

    def add_block(summed, block_index):
        offset = block_index * block_width
        row_block = lax.dynamic_slice_in_dim(value_grad, offset, block_width, 1)
        col_block = lax.dynamic_slice_in_dim(value_weight, offset, block_width, 1)
        product = lax.dot_general(row_block, col_block, (((1,), (1,)), ((), ())), preferred_element_type=jnp.float32)
        return (summed + rounded(product), None)
    start_sum = jnp.zeros((tokens, value_weight.shape[0]), jnp.float32)
    input_sum, unused = lax.scan(add_block, start_sum, jnp.arange(2 * KVH, dtype=jnp.int32))
    return (query_grad.reshape(tokens, KVH * GROUP * HD), key_grad.reshape(tokens, KVH * HD), input_sum.astype(jnp.bfloat16), value_grad)

def reference(hidden_in, value_weight, queries, key_rows, attention_out, output_grad, log_normalizer, document_ids):
    results = lax.map(partial(group_backward, value_weight), (hidden_in, queries, key_rows, attention_out, output_grad, log_normalizer, document_ids))
    query_grad, key_grad, input_grad, value_grad = results
    flat_inputs = hidden_in.reshape(-1, hidden_in.shape[2])
    flat_grads = value_grad.reshape(-1, value_grad.shape[2])
    value_weight_grad = lax.dot_general(flat_inputs, flat_grads, (((0,), (0,)), ((), ())), preferred_element_type=jnp.float32)
    return (query_grad, key_grad, input_grad, value_weight_grad)
```

```python
import math

import jax
import jax.numpy as jnp
from jax import lax
from jax.sharding import PartitionSpec as P


def swap(value, axis, mask):
    pairs = [(source, source ^ mask) for source in range(lax.axis_size(axis))]
    return lax.ppermute(value, axis, pairs)


def per_device(
    hidden_in,
    value_weight,
    queries,
    key_rows,
    attention_out,
    output_grad,
    log_normalizer,
    document_ids,
):
    f32 = jnp.float32
    bf16 = jnp.bfloat16
    tokens = hidden_in.shape[1]
    width = hidden_in.shape[2]
    head_count = log_normalizer.shape[2]
    half_width = key_rows.shape[2]
    head_width = 2 * half_width
    score_scale = 1.0 / math.sqrt(head_width)
    groups = lax.axis_size("dp")
    parts = lax.axis_size("tensor")
    chips = groups // 2
    block = width // groups
    token_block = tokens // parts
    group = lax.axis_index("dp")
    core = group % 2
    chip = group // 2
    part = lax.axis_index("tensor")
    lower_member = part % 2 == 0

    inputs_local = hidden_in[0]
    weight_t = value_weight.T
    key_half = key_rows[0].T
    other_key = swap(key_half, "tensor", 1)

    def parity_blocks(which):
        return jnp.concatenate(
            [
                lax.dynamic_slice_in_dim(inputs_local, (2 * index + which) * block, block, 1)
                for index in range(chips)
            ],
            1,
        )

    hidden_other = swap(parity_blocks(1 - core), "dp", 1)
    hidden_own = parity_blocks(core)

    weight_block = lax.dynamic_slice_in_dim(weight_t, group * block, block, 1)
    gathered = [swap(weight_block, "tensor", mask) for mask in range(1, parts)]
    gathered_other = [swap(piece, "dp", 1) for piece in gathered]
    weight_chip = lax.dynamic_slice_in_dim(weight_t, chip * (2 * block), 2 * block, 1)
    first_core = core == 0
    weight_rows = [weight_chip] + [
        jnp.where(
            first_core,
            jnp.concatenate([own, other], 1),
            jnp.concatenate([other, own], 1),
        )
        for own, other in zip(gathered, gathered_other)
    ]
    weight_full = jnp.concatenate(weight_rows, 0)

    value_half = lax.dot_general(
        weight_t, inputs_local, (((1,), (1,)), ((), ())), preferred_element_type=f32
    ).astype(bf16)
    other_value = swap(value_half, "tensor", 1)

    def joined(own, other):
        return jnp.where(
            lower_member,
            jnp.concatenate([own, other], 0),
            jnp.concatenate([other, own], 0),
        )

    keys_full = joined(key_half, other_key)
    values_full = joined(value_half, other_value)
    query_heads = queries[0].reshape(tokens, head_count, head_width)
    grad_heads = output_grad[0].reshape(tokens, head_count, head_width)
    out_heads = attention_out[0].reshape(tokens, head_count, head_width)
    position = jnp.arange(tokens, dtype=jnp.int32)
    documents = document_ids[0]
    allowed = (position[None, :] <= position[:, None]) & (documents[:, None] == documents[None, :])
    scores = jnp.einsum("thd,ds->hts", query_heads, keys_full, preferred_element_type=f32)
    normalizers = jnp.transpose(log_normalizer[0])[:, :, None]
    probabilities = jnp.where(allowed[None], jnp.exp(scores * score_scale - normalizers), 0.0)
    probs_low = probabilities.astype(bf16)
    value_part = jnp.einsum("hts,thd->ds", probs_low, grad_heads, preferred_element_type=f32)
    row_dots = jnp.einsum("thd,thd->ht", grad_heads, out_heads, preferred_element_type=f32)
    prob_grad = jnp.einsum("thd,ds->hts", grad_heads, values_full, preferred_element_type=f32)
    score_grad = (probabilities * (prob_grad - row_dots[:, :, None]) * score_scale).astype(bf16)
    query_grad = jnp.einsum("hts,ds->thd", score_grad, keys_full, preferred_element_type=f32)
    query_grad = query_grad.astype(bf16).reshape(1, tokens, head_count * head_width)
    key_part = jnp.einsum("hts,thd->ds", score_grad, query_heads, preferred_element_type=f32)

    def pair_sum(whole):
        low, high = whole[:half_width], whole[half_width:]
        got = swap(jnp.where(lower_member, high, low), "tensor", 1)
        return jnp.where(lower_member, low, high) + got

    value_grad = pair_sum(value_part).astype(bf16)
    key_grad = pair_sum(key_part).astype(bf16).T[None]
    value_grad_other = swap(value_grad, "dp", 1)

    weight_part = (
        jnp.dot(value_grad, hidden_own, preferred_element_type=f32)
        + jnp.dot(value_grad_other, hidden_other, preferred_element_type=f32)
    ).astype(bf16)

    def part_of(mask):
        return lax.dynamic_slice_in_dim(weight_part, (chip ^ mask) * block, block, 1)

    weight_sum = part_of(0).astype(f32)
    for piece in [swap(part_of(mask), "dp", 2 * mask) for mask in range(1, chips)]:
        weight_sum = weight_sum + piece.astype(f32)
    weight_grad = weight_sum.T

    def tokens_of(mask):
        return lax.dynamic_slice_in_dim(value_grad, (part ^ mask) * token_block, token_block, 1)

    rows = [tokens_of(0)] + [swap(tokens_of(mask), "tensor", mask) for mask in range(1, parts)]
    rows = jnp.concatenate(rows, 0)
    rows = jnp.concatenate([rows] + [swap(rows, "dp", 2 * mask) for mask in range(1, chips)], 1)
    product = lax.dot_general(
        rows, weight_full, (((0,), (0,)), ((), ())), preferred_element_type=f32
    ).astype(bf16)
    input_grad = jnp.zeros((token_block, width), bf16)
    for mask in range(chips):
        piece = product[mask * token_block : (mask + 1) * token_block]
        if mask:
            piece = swap(piece, "dp", 2 * mask)
        input_grad = lax.dynamic_update_slice_in_dim(
            input_grad, piece, (chip ^ mask) * (2 * block), 1
        )
    return (query_grad, key_grad, input_grad[None], weight_grad)


def solution(mesh):
    return jax.shard_map(
        per_device,
        mesh=mesh,
        in_specs=(
            P("dp", None, None),
            P(None, "tensor"),
            P("dp", None, "tensor"),
            P("dp", None, "tensor"),
            P("dp", None, "tensor"),
            P("dp", None, "tensor"),
            P("dp", None, "tensor"),
            P("dp", None),
        ),
        out_specs=(
            P("dp", None, "tensor"),
            P("dp", None, "tensor"),
            P("dp", "tensor", None),
            P("dp", "tensor"),
        ),
        check_vma=False,
    )
```

```python
import math

import jax
import jax.numpy as jnp
from jax import lax
from jax.experimental import pallas as pl
from jax.experimental.pallas import tpu as pltpu
from jax.sharding import PartitionSpec as P


F32 = jnp.float32
BF16 = jnp.bfloat16


def swap(value, axis, mask):
    pairs = [(source, source ^ mask) for source in range(lax.axis_size(axis))]
    return lax.ppermute(value, axis, pairs)


def contract(left, right, left_dim, right_dim):
    return lax.dot_general(
        left, right, (((left_dim,), (right_dim,)), ((), ())), preferred_element_type=F32
    )


def cost(micros):
    return pl.CostEstimate(flops=int(micros * 5e8), bytes_accessed=0, transcendentals=0)


def project_body(place, hidden, weight, value, send, rows, columns, sems, out_sems):
    count = sems.shape[1]
    block = rows.shape[1] // count
    loads, stores = [], []
    for index in range(count):
        lanes = pl.ds(index * block, block)
        pair = (
            pltpu.make_async_copy(hidden.at[:, lanes], rows.at[:, lanes], sems.at[0, index]),
            pltpu.make_async_copy(weight.at[:, lanes], columns.at[:, lanes], sems.at[1, index]),
        )
        for load in pair:
            load.start()
        loads.append(pair)
    total = jnp.zeros(value.shape, F32)
    for index in range(count):
        for load in loads[index]:
            load.wait()
        lanes = slice(index * block, (index + 1) * block)
        total += contract(columns[:, lanes], rows[:, lanes], 1, 1)
        if index % 2:
            start = pl.multiple_of((index - place[0]) * block, block)
            store = pltpu.make_async_copy(
                rows.at[:, pl.ds(start, block)],
                send.at[:, pl.ds(index // 2 * block, block)],
                out_sems.at[index // 2],
            )
            store.start()
            stores.append(store)
    value[...] = total.astype(BF16)
    for store in stores:
        store.wait()


def project(place, hidden, weight_t, block):
    tokens, width = hidden.shape
    columns = weight_t.shape[0]
    count = width // block
    return pl.pallas_call(
        project_body,
        in_specs=[
            pl.BlockSpec(memory_space=pltpu.SMEM),
            pl.BlockSpec(memory_space=pl.ANY),
            pl.BlockSpec(memory_space=pl.ANY),
        ],
        out_specs=[
            pl.BlockSpec(memory_space=pltpu.VMEM),
            pl.BlockSpec(memory_space=pl.ANY),
        ],
        scratch_shapes=[
            pltpu.VMEM((tokens, width), BF16),
            pltpu.VMEM((columns, width), BF16),
            pltpu.SemaphoreType.DMA((2, count)),
            pltpu.SemaphoreType.DMA((count // 2,)),
        ],
        out_shape=[
            jax.ShapeDtypeStruct((columns, tokens), BF16),
            jax.ShapeDtypeStruct((tokens, width // 2), BF16),
        ],
        cost_estimate=cost(5),
        name="project",
    )(place, hidden, weight_t)


def probabilities(query, norm, documents, keys, head):
    tokens = query.shape[0]
    width = keys.shape[0]
    rows = lax.broadcasted_iota(jnp.int32, (tokens, tokens), 0)
    columns = lax.broadcasted_iota(jnp.int32, (tokens, tokens), 1)
    names = jnp.broadcast_to(documents[...].astype(F32), (tokens, tokens))
    allowed = (columns <= rows) & (names == names.T)
    scores = contract(query[:, head * width : (head + 1) * width], keys, 1, 0)
    scores = scores * (1.0 / math.sqrt(width))
    return jnp.where(allowed, jnp.exp(scores - norm[:, head : head + 1]), 0.0)


def joined(place, target, own, other):
    half = own.shape[0]
    target[pl.ds(pl.multiple_of(place[1] * half, half), half), :] = own[...]
    target[pl.ds(pl.multiple_of((1 - place[1]) * half, half), half), :] = other[...]
    return target[...]


def split(place, source, keep, send):
    half = keep.shape[0]
    keep[...] = source[pl.ds(pl.multiple_of(place[1] * half, half), half), :]
    send[...] = source[pl.ds(pl.multiple_of((1 - place[1]) * half, half), half), :]


def values_body(
    place, query, grad, key_own, key_other, norm, documents, keep, send, keys, part
):
    width = keys.shape[0]
    key_t = joined(place, keys, key_own, key_other)
    norm_t = norm[...].T
    total = jnp.zeros(part.shape, F32)
    for head in range(norm.shape[0]):
        probs = probabilities(query, norm_t, documents, key_t, head)
        g = grad[:, head * width : (head + 1) * width]
        total += contract(g, probs.astype(BF16), 0, 0)
    part[...] = total
    split(place, part, keep, send)


def scores_body(
    place, query, grad, out, key_own, key_other, value_own, value_other, norm, documents,
    query_grad, keep, send, keys, values, part,
):
    width = keys.shape[0]
    scale = 1.0 / math.sqrt(width)
    key_t = joined(place, keys, key_own, key_other)
    value_t = joined(place, values, value_own, value_other)
    norm_t = norm[...].T
    total = jnp.zeros(part.shape, F32)
    for head in range(norm.shape[0]):
        probs = probabilities(query, norm_t, documents, key_t, head)
        lanes = slice(head * width, (head + 1) * width)
        g = grad[:, lanes]
        dots = jnp.sum(g.astype(F32) * out[:, lanes].astype(F32), axis=1, keepdims=True)
        score_grad = (probs * (contract(g, value_t, 1, 0) - dots) * scale).astype(BF16)
        query_grad[:, lanes] = contract(score_grad, key_t, 1, 1).astype(BF16)
        total += contract(query[:, lanes], score_grad, 0, 0)
    part[...] = total
    split(place, part, keep, send)


def attend(body, place, operands, half, joins, extra=()):
    tokens = operands[0].shape[0]
    vmem = pl.BlockSpec(memory_space=pltpu.VMEM)
    halves = [jax.ShapeDtypeStruct((half, tokens), F32)] * 2
    return pl.pallas_call(
        body,
        in_specs=[pl.BlockSpec(memory_space=pltpu.SMEM)] + [vmem] * len(operands),
        out_specs=[vmem] * (len(extra) + 2),
        scratch_shapes=[pltpu.VMEM((2 * half, tokens), BF16)] * joins
        + [pltpu.VMEM((2 * half, tokens), F32)],
        out_shape=list(extra) + halves,
        cost_estimate=cost(3),
    )(place, *operands)


def weight_body(place, value_own, value_other, hidden, hidden_other, *rest):
    *outs, own, other, sems = rest
    block = outs[0].shape[1]
    loads = []
    for index in range(len(outs)):
        chip = place[2] ^ index
        from_own = pl.multiple_of((2 * chip + place[0]) * block, block)
        from_other = pl.multiple_of(chip * block, block)
        pair = (
            pltpu.make_async_copy(
                hidden.at[:, pl.ds(from_own, block)], own.at[index], sems.at[0, index]
            ),
            pltpu.make_async_copy(
                hidden_other.at[:, pl.ds(from_other, block)], other.at[index], sems.at[1, index]
            ),
        )
        for load in pair:
            load.start()
        loads.append(pair)
    values = jnp.concatenate([value_own[...], value_other[...]], 1)
    for index, out in enumerate(outs):
        for load in loads[index]:
            load.wait()
        rows = jnp.concatenate([own[index], other[index]], 0)
        out[...] = contract(values, rows, 1, 0).astype(BF16)


def weight_parts(place, value_own, value_other, hidden, hidden_other, block):
    columns, tokens = value_own.shape
    chips = hidden.shape[1] // (2 * block)
    vmem = pl.BlockSpec(memory_space=pltpu.VMEM)
    return pl.pallas_call(
        weight_body,
        in_specs=[
            pl.BlockSpec(memory_space=pltpu.SMEM),
            vmem,
            vmem,
            pl.BlockSpec(memory_space=pl.ANY),
            pl.BlockSpec(memory_space=pl.ANY),
        ],
        out_specs=[vmem] * chips,
        scratch_shapes=[
            pltpu.VMEM((chips, tokens, block), BF16),
            pltpu.VMEM((chips, tokens, block), BF16),
            pltpu.SemaphoreType.DMA((2, chips)),
        ],
        out_shape=[jax.ShapeDtypeStruct((columns, block), BF16)] * chips,
        cost_estimate=cost(4),
        name="weight_parts",
    )(place, value_own, value_other, hidden, hidden_other)


def input_body(counts, place, *refs):
    chips, parts = counts
    rows = jnp.concatenate([ref[...] for ref in refs[:chips]], 0)
    own = refs[chips]
    pieces = refs[chips + 1 : chips + parts]
    pieces_other = refs[chips + parts : chips + 2 * parts - 1]
    outs = refs[chips + 2 * parts - 1 : -2]
    columns, sem = refs[-2:]
    block = pieces[0].shape[1]
    start = pl.multiple_of(place[2] * (2 * block), 2 * block)
    load = pltpu.make_async_copy(own.at[:, pl.ds(start, 2 * block)], columns, sem)
    load.start()
    load.wait()
    size = outs[0].shape[0]
    for far, group in ((0, pieces), (1, pieces_other)):
        side = place[0] if far == 0 else 1 - place[0]
        lanes = pl.ds(pl.multiple_of(side * block, block), block)
        weights = jnp.concatenate([columns[:, lanes]] + [ref[...] for ref in group], 0)
        product = contract(rows, weights, 1, 0).astype(BF16)
        for index, out in enumerate(outs):
            out[:, lanes] = product[index * size : (index + 1) * size]


def input_parts(place, rows, weight_t, pieces, pieces_other):
    size = rows[0].shape[0]
    columns, block = pieces[0].shape
    vmem = pl.BlockSpec(memory_space=pltpu.VMEM)
    return pl.pallas_call(
        lambda *refs: input_body((len(rows), len(pieces) + 1), *refs),
        in_specs=[pl.BlockSpec(memory_space=pltpu.SMEM)]
        + [vmem] * len(rows)
        + [pl.BlockSpec(memory_space=pl.ANY)]
        + [vmem] * (2 * len(pieces)),
        out_specs=[vmem] * len(rows),
        scratch_shapes=[pltpu.VMEM((columns, 2 * block), BF16), pltpu.SemaphoreType.DMA],
        out_shape=[jax.ShapeDtypeStruct((size, 2 * block), BF16)] * len(rows),
        cost_estimate=cost(4),
        name="input_parts",
    )(place, *rows, weight_t, *pieces, *pieces_other)


def per_device(
    hidden_in,
    value_weight,
    queries,
    key_rows,
    attention_out,
    output_grad,
    log_normalizer,
    document_ids,
):
    tokens = hidden_in.shape[1]
    width = hidden_in.shape[2]
    half_width = key_rows.shape[2]
    groups = lax.axis_size("dp")
    parts = lax.axis_size("tensor")
    chips = groups // 2
    block = width // groups
    token_block = tokens // parts
    group = lax.axis_index("dp")
    core = group % 2
    chip = group // 2
    part = lax.axis_index("tensor")
    place = jnp.stack([core, part % 2, chip, part]).astype(jnp.int32)

    inputs_local = hidden_in[0]
    weight_t = value_weight.T
    key_half = key_rows[0].T
    norm = log_normalizer[0].T

    held = {0: lax.dynamic_slice_in_dim(weight_t, group * block, block, 1)}
    for mask in far_first(parts):
        for seen in list(held):
            held[seen ^ mask] = swap(held[seen], "tensor", mask)
    pieces = [held[mask] for mask in range(1, parts)]
    pieces_other = [swap(held[mask], "dp", 1) for mask in range(1, parts)]

    other_key = swap(key_half, "tensor", 1)
    value_half, hidden_send = project(place, inputs_local, weight_t, block)
    hidden_other = swap(hidden_send, "dp", 1)
    query, grad = queries[0], output_grad[0]
    keep, send = attend(
        values_body, place,
        (query, grad, key_half, other_key, norm, document_ids), half_width, 1,
    )
    value_grad = (keep + swap(send, "tensor", 1)).astype(BF16)
    value_grad_other = swap(value_grad, "dp", 1)
    value_rows = value_grad.T

    weight_out = weight_parts(
        place, value_grad, value_grad_other, inputs_local, hidden_other, block
    )
    weight_sum = weight_out[0].astype(F32)
    for mask in range(1, chips):
        weight_sum = weight_sum + swap(weight_out[mask], "dp", 2 * mask).astype(F32)
    weight_grad = weight_sum.T

    def tokens_of(mask):
        start = (part ^ mask) * token_block
        return lax.dynamic_slice_in_dim(value_rows, start, token_block, 0)

    rows = [tokens_of(0)]
    rows += [swap(tokens_of(mask), "tensor", mask) for mask in range(1, parts)]
    rows = jnp.concatenate(rows, 1)
    rows = [rows] + [swap(rows, "dp", 2 * mask) for mask in range(1, chips)]
    product = input_parts(place, rows, weight_t, pieces, pieces_other)
    input_grad = jnp.zeros((token_block, width), BF16)
    for mask in range(chips):
        value = swap(product[mask], "dp", 2 * mask) if mask else product[0]
        input_grad = lax.dynamic_update_slice_in_dim(
            input_grad, value, (chip ^ mask) * (2 * block), 1
        )

    other_value = swap(value_half, "tensor", 1)
    query_grad, keep, send = attend(
        scores_body, place,
        (
            query, grad, attention_out[0], key_half, other_key, value_half, other_value,
            norm, document_ids,
        ),
        half_width, 2, (jax.ShapeDtypeStruct(query.shape, BF16),),
    )
    key_grad = (keep + swap(send, "tensor", 1)).astype(BF16).T[None]
    return (query_grad[None], key_grad, input_grad[None], weight_grad)


def far_first(count):
    return [1 << bit for bit in reversed(range(count.bit_length() - 1))]


def solution(mesh):
    return jax.shard_map(
        per_device,
        mesh=mesh,
        in_specs=(
            P("dp", None, None),
            P(None, "tensor"),
            P("dp", None, "tensor"),
            P("dp", None, "tensor"),
            P("dp", None, "tensor"),
            P("dp", None, "tensor"),
            P("dp", None, "tensor"),
            P("dp", None),
        ),
        out_specs=(
            P("dp", None, "tensor"),
            P("dp", None, "tensor"),
            P("dp", "tensor", None),
            P("dp", "tensor"),
        ),
        check_vma=False,
    )
```
